32 devices in a mesh: freq: 8 (over z, x), sens: 4 (over y, core).
Axes of the slice: x: 2, y: 2, z: 4, core: 2. Of those that a mesh axis runs over, the one named last changes fastest.
Arguments:
- samples: bfloat16 [128, 608, 420], P('freq', 'sens'), may hold values from -6 to 6
- response_tiles: bfloat16 [448, 2, 608, 21], P('freq', None, 'sens'), may hold values from -0.25 to 0.25
- slot_sensor: int32 [608], P('sens'), may hold values from -1 to 599, as said below
- sensor_noise: float32 [600], replicated, may hold values from 0.02 to 5
- advance_offset: int32 [21], replicated, may hold values from 0 to 419
Outputs:
- outlook_values: bfloat16 [128, 21, 420], P('freq')
- noise_spread: float32 [21], replicated
The draws below stay inside these ranges and needn't reach their ends.
Inputs may be any that keep to these rules, and one draw needn't show every extreme that they name: `slot_sensor`: every sensor number appears in exactly one slot; the other 8 slots hold -1.
All inputs are finite; a program needn't handle non-finite values.
Results may differ from the reference program's by a relative error of at most 0.0055.
Values may be sent and summed in bfloat16 or wider, within the bound.
A program may use at most 64 MiB of HBM per device.

```python
import math
import jax
import jax.numpy as jnp
from jax import lax

TARGET_PLACES = 21
PROBE_COUNT = 600
HORIZON_LENGTH = 420
KEPT_HARMONICS = 448
POSTERIOR_COUNT = 128
PROBE_POSITIONS = 608
N_FREQ = 8


def draw_slot_sensor(key, part):
    ordering = jax.random.permutation(key, PROBE_POSITIONS).astype(jnp.int32)
    return jnp.where(ordering < PROBE_COUNT, ordering, -1).astype(jnp.int32)


def place_ends(drawn, rng, least, largest):
    spot = [jax.random.randint(jax.random.fold_in(rng, axis), (), 0, length) for axis, length in enumerate(drawn.shape)]
    main_axis = drawn.shape.index(max(drawn.shape))
    beside = spot[:main_axis] + [(spot[main_axis] + 1) % drawn.shape[main_axis]] + spot[main_axis + 1:]
    return drawn.at[tuple(spot)].set(least).at[tuple(beside)].set(largest)


def block_scale(own_key, dims, pieces, low, high):
    def one(position, blocks):
        draws = jax.random.uniform(jax.random.fold_in(jax.random.fold_in(own_key, 6), position), (blocks,), jnp.float32, low / len(pieces), high / len(pieces))
        return jnp.repeat(jnp.exp(draws), dims[position] // blocks).reshape((-1,) + (1,) * (len(dims) - position - 1))

    level = one(*pieces[0])
    for cut in pieces[1:]:
        level = level * one(*cut)
    return level


def noise(own_key, shape, spread, bound, shards=(), held_as=jnp.bfloat16):
    gain = block_scale(own_key, shape, shards, -0.22, 0.18) if shards else 1.0
    array = jax.random.normal(own_key, shape, jnp.float32) * spread * gain
    return jnp.minimum(jnp.maximum(array, -bound), bound).astype(held_as)


def setup_inputs(seed: int = 0) -> dict:
    splits = jax.random.split(jax.random.key(seed), 6)
    return {
        "samples": noise(splits[0], (POSTERIOR_COUNT, PROBE_POSITIONS, HORIZON_LENGTH), 1.0, 6.0, ((0, 8), (1, 4))),
        "response_tiles": noise(splits[1], (KEPT_HARMONICS, 2, PROBE_POSITIONS, TARGET_PLACES), (PROBE_COUNT * HORIZON_LENGTH // KEPT_HARMONICS) ** -0.5, 0.25, ((0, 8), (2, 4))),
        "slot_sensor": draw_slot_sensor(jax.random.fold_in(splits[5], 71), 0),
        "sensor_noise": jnp.clip(jnp.exp(jax.random.uniform(splits[3], (PROBE_COUNT,), jnp.float32, math.log(0.02), math.log(5.0))), 0.02, 5.0),
        "advance_offset": place_ends(jax.random.randint(splits[4], (TARGET_PLACES,), 0, HORIZON_LENGTH), jax.random.fold_in(splits[4], 1), 0, HORIZON_LENGTH - 1).astype(jnp.int32),
    }


def angles(first_bin, bin_count, period, factor):
    bin_index = first_bin + lax.iota(jnp.int32, bin_count)
    turn_count = (bin_index[:, None] * factor[None, :]) % period
    return turn_count.astype(jnp.float32) * (2.0 * math.pi / period)


def forward_table(bin_count, step_count, period):
    phase_angle = angles(0, bin_count, period, lax.iota(jnp.int32, step_count))
    return jnp.stack([jnp.cos(phase_angle), -jnp.sin(phase_angle)]).astype(jnp.bfloat16)


def inverse_table(bin_count, step_count, period):
    bin_index = lax.iota(jnp.int32, bin_count)
    weight = jnp.where(bin_index == 0, 1.0, 2.0).astype(jnp.float32) / period
    phase_angle = angles(0, bin_count, period, lax.iota(jnp.int32, step_count))
    return jnp.stack([weight[:, None] * jnp.cos(phase_angle), -weight[:, None] * jnp.sin(phase_angle)])


def reference(samples, response_tiles, slot_sensor, sensor_noise, advance_offset):
    period = 2 * KEPT_HARMONICS
    highest = lax.Precision.HIGHEST
    live_slot = (slot_sensor >= 0).astype(jnp.bfloat16)
    blocks = response_tiles * live_slot[None, None, :, None]
    wide = blocks.astype(jnp.float32)
    sensor_ids = lax.iota(jnp.int32, PROBE_COUNT)
    slot_noise = jnp.sum(jnp.where(slot_sensor[:, None] == sensor_ids[None, :], sensor_noise[None, :], jnp.float32(0.0)), axis=1)
    power = wide[:, 0] * wide[:, 0] + wide[:, 1] * wide[:, 1]
    bin_index = lax.iota(jnp.int32, KEPT_HARMONICS)
    bin_weight = jnp.where(bin_index == 0, 1.0, 2.0).astype(jnp.float32) / period
    per_bin = jnp.einsum("ksq,s->kq", power, slot_noise, precision=highest)
    noise_spread = jnp.dot(bin_weight, per_bin, precision=highest)

    forward_flat = forward_table(KEPT_HARMONICS, HORIZON_LENGTH, period).reshape(2 * KEPT_HARMONICS, HORIZON_LENGTH)
    backward = inverse_table(KEPT_HARMONICS, HORIZON_LENGTH, period).astype(jnp.float32)
    block_real = wide[:, 0]
    block_imag = wide[:, 1]
    twiddle = angles(0, KEPT_HARMONICS, period, advance_offset)
    cosine = jnp.cos(twiddle)[:, :, None]
    sine_part = jnp.sin(twiddle)[:, :, None]

    def product(left, right):
        return jnp.einsum("krs,ksq->kqr", left, right, precision=highest)

    def single_block(sample_block):
        row_count = sample_block.shape[0]
        flat_out = jnp.dot(sample_block.reshape(row_count * PROBE_POSITIONS, HORIZON_LENGTH), forward_flat.T, preferred_element_type=jnp.float32)
        spectra = flat_out.reshape(row_count, PROBE_POSITIONS, 2, KEPT_HARMONICS).transpose(2, 3, 0, 1).astype(jnp.bfloat16)
        spec_real = spectra[0].astype(jnp.float32)
        spec_imag = spectra[1].astype(jnp.float32)
        real_part = product(spec_real, block_real) - product(spec_imag, block_imag)
        imag_part = product(spec_real, block_imag) + product(spec_imag, block_real)
        shifted = jnp.stack([real_part * cosine - imag_part * sine_part, real_part * sine_part + imag_part * cosine])
        return jnp.einsum("ckqr,ckt->rqt", shifted, backward, precision=highest).astype(jnp.bfloat16)

    estimate_tiles = lax.map(single_block, samples.reshape(N_FREQ, POSTERIOR_COUNT // N_FREQ, PROBE_POSITIONS, HORIZON_LENGTH))
    outlook_values = estimate_tiles.reshape(POSTERIOR_COUNT, TARGET_PLACES, HORIZON_LENGTH)
    return (outlook_values, noise_spread)
```

```python
import functools
import math

import jax
import jax.numpy as jnp
import numpy as np
from jax import lax
from jax.experimental import pallas as pl
from jax.experimental.pallas import tpu as pltpu
from jax.sharding import PartitionSpec as P

MESH = pl.DeviceIdType.MESH
HALF = 64
LANES = 128


def make_tables(freq_size, bins_dev, step_count, group, chunks):
    bin_count = freq_size * bins_dev
    period = 2 * bin_count
    slot = np.arange(freq_size * chunks * group)
    block, inside = slot // (chunks * group), slot % (chunks * group)
    live = (inside < bins_dev).astype(np.float64)
    bins = np.where(inside < bins_dev, block * bins_dev + inside, 0)
    turns = bins[:, None] * np.arange(step_count)[None, :] % period
    angle = turns * (2.0 * math.pi / period)
    forward = np.stack([np.cos(angle), -np.sin(angle)]) * live[None, :, None]
    weight = np.where(bins == 0, 1.0, 2.0) / period * live
    inverse = np.stack([np.cos(angle), -np.sin(angle)]) * weight[None, :, None]
    inverse = inverse.reshape(2, freq_size * chunks, group, step_count).transpose(0, 2, 1, 3)
    inverse = inverse.reshape(2 * group * freq_size * chunks, step_count)
    return bins, weight, forward, inverse


def kernel(
    dims,
    tiles, samples, forward, slot_noise, noise_weight, cosine, sine, inverse,
    out, spread,
    held, spectra, z_own, z_send, z_recv, gathered, spread_send, spread_recv,
    own_sem, ring_send, ring_recv, z_send_sem, z_recv_sem, s_send_sem, s_recv_sem,
):
    freq_size, sens_size, chunks, group, sites, count = dims
    rows, slots, step_count = samples.shape
    all_chunks = freq_size * chunks
    per_bin = 2 * rows
    lane_tiles = spectra.shape[0]
    me_f = lax.axis_index("freq")
    me_s = lax.axis_index("sens")
    n = freq_size

    def position_of(index):
        odd, pair = lax.rem(index, 2), index // 2
        return pair * (1 - odd) + (n - 1 - pair) * odd

    def index_of(position):
        high = position // (n // 2)
        return 2 * position * (1 - high) + (2 * (n - 1 - position) + 1) * high

    me_p = position_of(me_f)

    def along(step):
        return index_of(lax.rem(me_p + step + 2 * n, n))

    right, left = along(1), along(-1)
    barrier = pltpu.get_barrier_semaphore()
    for neighbour in (left, right):
        pl.semaphore_signal(barrier, inc=1, device_id={"freq": neighbour}, device_id_type=MESH)
    for d in range(1, sens_size):
        peer = lax.rem(me_s + d, sens_size)
        pl.semaphore_signal(barrier, inc=1, device_id={"sens": peer}, device_id_type=MESH)
    pl.semaphore_wait(barrier, 2 + sens_size - 1)

    cuts = [chunks * i // count for i in range(count + 1)]
    half = count // 2
    pieces = [j for i in range(half) for j in (i, half + i) if cuts[j + 1] > cuts[j]]
    sign_of = (1,) * half + (-1,) * half

    def ring_copy(step, j, received):
        d = sign_of[j]
        low, size = cuts[j], cuts[j + 1] - cuts[j]
        origin = along(-d * (step + (1 if received else 0)))
        block = held.at[origin, pl.ds(low, size)]
        source = tiles.at[pl.ds(low, size)] if step == 0 and not received else block
        return pltpu.make_async_remote_copy(
            src_ref=source, dst_ref=block,
            send_sem=ring_send.at[j, step], recv_sem=ring_recv.at[j, step],
            device_id={"freq": right if d == 1 else left}, device_id_type=MESH,
        )

    for j in pieces:
        ring_copy(0, j, False).start()
    own = pltpu.make_async_copy(tiles, held.at[me_f], own_sem)
    own.start()
    own.wait()

    lane = lax.broadcasted_iota(jnp.int32, (rows, LANES), 1)
    which = (lane % HALF) // sites
    sign = jnp.where(lane < HALF, -1.0, 1.0).astype(jnp.float32)
    spread[...] = jnp.zeros_like(spread)

    def transform(r):
        for c in range(2):
            value = lax.dot_general(
                forward[c], samples[r], (((1,), (1,)), ((), ())),
                preferred_element_type=jnp.float32,
            )
            for tile in range(lane_tiles):
                part = value[:, tile * LANES:min(slots, (tile + 1) * LANES)]
                if part.shape[1] < LANES:
                    part = jnp.concatenate(
                        [part, jnp.zeros((part.shape[0], LANES - part.shape[1]), part.dtype)], axis=1
                    )
                spectra[tile, pl.ds(c * rows + r, part.shape[0], stride=per_bin), :] = part

    def contract(origin, j):
        def body(chunk, carry):
            at = origin * chunks + chunk
            weights = held[origin, chunk]
            first = pl.multiple_of(at * (group * per_bin), group * per_bin)
            parts = [spectra[tile, pl.ds(first, group * per_bin), :] for tile in range(lane_tiles)]
            spec = jnp.concatenate(parts, axis=1)[:, :slots].astype(jnp.bfloat16)
            product = jnp.dot(spec, weights, preferred_element_type=jnp.float32)
            picked = [product[c * rows:(c + 1) * rows] for c in range(2)]
            for i in range(1, group):
                for c in range(2):
                    low = i * per_bin + c * rows
                    picked[c] = jnp.where(which == i, product[low:low + rows], picked[c])
            value = picked[0] + sign * pltpu.roll(picked[1], HALF, 1)
            z_own[pl.ds(pl.multiple_of(at * rows, rows), rows), :] = value
            z_send[at] = value.astype(jnp.bfloat16)
            wide = weights.astype(jnp.float32)
            power = wide * wide * slot_noise[...]
            total = power.reshape(slots // 8, 8, LANES).sum(axis=0)
            spread[...] += total * noise_weight[pl.ds(at, 1), :]
            return carry

        lax.fori_loop(cuts[j], cuts[j + 1], body, 0)

    def z_copies(step, j):
        origin = along(-sign_of[j] * step)
        part = pl.ds(origin * chunks + cuts[j], cuts[j + 1] - cuts[j])
        return [
            pltpu.make_async_remote_copy(
                src_ref=z_send.at[part], dst_ref=z_recv.at[d - 1, part],
                send_sem=z_send_sem.at[d - 1, step * count + j],
                recv_sem=z_recv_sem.at[d - 1, step * count + j],
                device_id={"sens": lax.rem(me_s + d, sens_size)}, device_id_type=MESH,
            )
            for d in range(1, sens_size)
        ]

    tasks = [("transform", r) for r in range(rows)] + [("contract", 0, j) for j in pieces]
    waiting = []

    def flush():
        while waiting:
            for copy in z_copies(*waiting.pop(0)):
                copy.start()

    def run(task):
        if task[0] == "transform":
            transform(task[1])
            return
        _, step, j = task
        contract(along(-sign_of[j] * step), j)
        flush()
        waiting.append((step, j))

    def budget(count):
        for _ in range(min(count, len(tasks))):
            run(tasks.pop(0))

    budget(2)
    for step in range(n - 1):
        for j in pieces:
            ring_copy(step, j, True).wait_recv()
            if step < n - 2:
                ring_copy(step + 1, j, False).start()
            tasks.append(("contract", step + 1, j))
            budget(2)
    budget(len(tasks))
    flush()
    spread_send[...] = spread[...]
    spread_copies = [
        pltpu.make_async_remote_copy(
            src_ref=spread_send, dst_ref=spread_recv.at[d - 1],
            send_sem=s_send_sem.at[d - 1], recv_sem=s_recv_sem.at[d - 1],
            device_id={"sens": lax.rem(me_s + d, sens_size)}, device_id_type=MESH,
        )
        for d in range(1, sens_size)
    ]
    for copy in spread_copies:
        copy.start()
    for step in range(n - 1):
        for j in pieces:
            ring_copy(step, j, False).wait_send()
    for step in range(n):
        for j in pieces:
            for copy in z_copies(step, j):
                copy.wait()
    for copy in spread_copies:
        copy.wait()
    total = spread[...]
    for d in range(1, sens_size):
        total += spread_recv[d - 1]
    spread[...] = total

    def combine(at, carry):
        here = pl.ds(pl.multiple_of(at * rows, rows), rows)
        value = z_own[here, :]
        for d in range(1, sens_size):
            value += z_recv[d - 1, at].astype(jnp.float32)
        z_own[here, :] = value * cosine[pl.ds(at, 1), :] + pltpu.roll(value, HALF, 1) * sine[pl.ds(at, 1), :]
        return carry

    lax.fori_loop(0, all_chunks, combine, 0, unroll=4)

    seat = 32
    together = LANES // seat
    place = lax.broadcasted_iota(jnp.int32, (all_chunks, LANES), 1) // seat
    for base in range(0, rows, together):
        mine = [z_own[pl.ds(base + m, all_chunks, stride=rows), :] for m in range(together)]
        for c in range(2):
            for i in range(group):
                start = c * HALF + i * sites
                value = None
                for m in range(together):
                    moved = pltpu.roll(mine[m], (m * seat - start) % LANES, 1)
                    value = moved if value is None else jnp.where(place == m, moved, value)
                low = (c * group + i) * all_chunks
                gathered[low:low + all_chunks, base * seat:(base + together) * seat] = value.astype(jnp.bfloat16)
    result = lax.dot_general(
        gathered[...], inverse[...], (((0,), (0,)), ((), ())), preferred_element_type=jnp.float32
    )
    for r in range(rows):
        out[r] = result[r * seat:r * seat + sites].astype(jnp.bfloat16)


def on_device(freq_size, sens_size, samples, response_tiles, slot_sensor, sensor_noise, advance_offset):
    bins_dev, _, slots, sites = response_tiles.shape
    rows, _, step_count = samples.shape
    group = HALF // sites
    chunks = -(-bins_dev // group)
    all_chunks = freq_size * chunks
    period = 2 * freq_size * bins_dev
    bins, weight, forward, inverse = make_tables(freq_size, bins_dev, step_count, group, chunks)

    def per_lane(table):
        table = table.reshape(all_chunks, group * sites)
        table = jnp.pad(table, ((0, 0), (0, HALF - group * sites)))
        return jnp.concatenate([table, table], axis=1)

    live_slot = slot_sensor >= 0
    sensor_ids = lax.iota(jnp.int32, sensor_noise.shape[0])
    slot_noise = jnp.sum(
        jnp.where(slot_sensor[:, None] == sensor_ids[None, :], sensor_noise[None, :], jnp.float32(0.0)),
        axis=1,
    )
    slot_noise = jnp.broadcast_to(slot_noise[:, None], (slots, LANES))
    tiles = jnp.where(live_slot[None, None, :, None], response_tiles, jnp.bfloat16(0))
    tiles = jnp.pad(tiles, ((0, chunks * group - bins_dev), (0, 0), (0, 0), (0, 0)))
    tiles = tiles.reshape(chunks, group, 2, slots, sites).transpose(0, 3, 2, 1, 4)
    tiles = tiles.reshape(chunks, slots, 2, group * sites)
    tiles = jnp.pad(tiles, ((0, 0), (0, 0), (0, 0), (0, HALF - group * sites))).reshape(chunks, slots, LANES)

    turns = jnp.asarray(bins, jnp.int32)[:, None] * advance_offset[None, :] % period
    twiddle = turns.astype(jnp.float32) * (2.0 * math.pi / period)
    lane_sign = jnp.where(lax.iota(jnp.int32, LANES) < HALF, -1.0, 1.0).astype(jnp.float32)
    cosine = per_lane(jnp.cos(twiddle))
    sine = per_lane(jnp.sin(twiddle)) * lane_sign[None, :]
    noise_weight = per_lane(jnp.asarray(np.repeat(weight[:, None], sites, axis=1), jnp.float32))

    lane_tiles = -(-slots // LANES)
    peers = sens_size - 1
    count = 4 if peers * freq_size * 4 <= 1024 else 2
    vmem = pl.BlockSpec(memory_space=pltpu.VMEM)
    outlook, spread = pl.pallas_call(
        functools.partial(kernel, (freq_size, sens_size, chunks, group, sites, count)),
        out_shape=(
            jax.ShapeDtypeStruct((rows, sites, step_count), jnp.bfloat16),
            jax.ShapeDtypeStruct((8, LANES), jnp.float32),
        ),
        in_specs=[vmem] * 8,
        out_specs=(vmem, vmem),
        scratch_shapes=[
            pltpu.VMEM((freq_size, chunks, slots, LANES), jnp.bfloat16),
            pltpu.VMEM((lane_tiles, all_chunks * group * 2 * rows, LANES), jnp.float32),
            pltpu.VMEM((all_chunks * rows, LANES), jnp.float32),
            pltpu.VMEM((all_chunks, rows, LANES), jnp.bfloat16),
            pltpu.VMEM((peers, all_chunks, rows, LANES), jnp.bfloat16),
            pltpu.VMEM((2 * group * all_chunks, rows * 32), jnp.bfloat16),
            pltpu.VMEM((8, LANES), jnp.float32),
            pltpu.VMEM((peers, 8, LANES), jnp.float32),
            pltpu.SemaphoreType.DMA,
            pltpu.SemaphoreType.DMA((count, freq_size - 1)),
            pltpu.SemaphoreType.DMA((count, freq_size - 1)),
            pltpu.SemaphoreType.DMA((peers, freq_size * count)),
            pltpu.SemaphoreType.DMA((peers, freq_size * count)),
            pltpu.SemaphoreType.DMA((peers,)),
            pltpu.SemaphoreType.DMA((peers,)),
        ],
        compiler_params=pltpu.CompilerParams(
            collective_id=0, has_side_effects=True, vmem_limit_bytes=60 * 1024 * 1024
        ),
    )(
        tiles, samples, jnp.asarray(forward, jnp.bfloat16), slot_noise, noise_weight,
        cosine, sine, jnp.asarray(inverse, jnp.bfloat16),
    )
    by_lane = jnp.sum(spread, axis=0)
    halves = by_lane[:group * sites] + by_lane[HALF:HALF + group * sites]
    noise_spread = jnp.sum(halves.reshape(group, sites), axis=0)
    return (outlook, noise_spread)


def solution(mesh):
    placed = (P("freq", "sens", None), P("freq", None, "sens", None), P("sens"), P(), P())
    return jax.shard_map(
        functools.partial(on_device, mesh.shape["freq"], mesh.shape["sens"]),
        mesh=mesh,
        in_specs=placed,
        out_specs=(P("freq", None, None), P()),
        check_vma=False,
    )
```

```python
import functools
import math

import jax
import jax.numpy as jnp
import numpy as np
from jax import lax
from jax.experimental import pallas as pl
from jax.experimental.pallas import tpu as pltpu
from jax.sharding import PartitionSpec as P

MESH = pl.DeviceIdType.MESH
HALF = 64
LANES = 128


def make_tables(freq_size, bins_dev, step_count, group, chunks):
    bin_count = freq_size * bins_dev
    period = 2 * bin_count
    slot = np.arange(freq_size * chunks * group)
    block, inside = slot // (chunks * group), slot % (chunks * group)
    live = (inside < bins_dev).astype(np.float64)
    bins = np.where(inside < bins_dev, block * bins_dev + inside, 0)
    turns = bins[:, None] * np.arange(step_count)[None, :] % period
    angle = turns * (2.0 * math.pi / period)
    forward = np.stack([np.cos(angle), -np.sin(angle)]) * live[None, :, None]
    weight = np.where(bins == 0, 1.0, 2.0) / period * live
    inverse = np.stack([np.cos(angle), -np.sin(angle)]) * weight[None, :, None]
    inverse = inverse.reshape(2, freq_size * chunks, group, step_count).transpose(0, 2, 1, 3)
    inverse = inverse.reshape(2 * group * freq_size * chunks, step_count)
    return bins, weight, forward, inverse


def kernel(
    dims,
    tiles, samples, forward, slot_facts, sorter, noise_weight, cosine, sine, inverse,
    out, spread,
    held, spectra, z_own, z_send, z_recv, gathered, spread_send, spread_recv,
    ring_send, ring_recv, z_send_sem, z_recv_sem, s_send_sem, s_recv_sem,
):
    freq_size, sens_size, chunks, group, sites, count = dims
    rows, slots, step_count = samples.shape
    all_chunks = freq_size * chunks
    per_bin = 2 * rows
    lane_tiles = spectra.shape[0]
    me_f = lax.axis_index("freq")
    me_s = lax.axis_index("sens")
    n = freq_size

    def position_of(index):
        odd, pair = lax.rem(index, 2), index // 2
        return pair * (1 - odd) + (n - 1 - pair) * odd

    def index_of(position):
        high = position // (n // 2)
        return 2 * position * (1 - high) + (2 * (n - 1 - position) + 1) * high

    me_p = position_of(me_f)

    def along(step):
        return index_of(lax.rem(me_p + step + 2 * n, n))

    right, left = along(1), along(-1)
    barrier = pltpu.get_barrier_semaphore()
    for neighbour in (left, right):
        pl.semaphore_signal(barrier, inc=1, device_id={"freq": neighbour}, device_id_type=MESH)
    for d in range(1, sens_size):
        peer = lax.rem(me_s + d, sens_size)
        pl.semaphore_signal(barrier, inc=1, device_id={"sens": peer}, device_id_type=MESH)

    cuts = [chunks * i // count for i in range(count + 1)]
    half = count // 2
    pieces = [j for i in range(half) for j in (i, half + i) if cuts[j + 1] > cuts[j]]
    sign_of = (1,) * half + (-1,) * half

    def ring_copy(step, j, received):
        d = sign_of[j]
        low, size = cuts[j], cuts[j + 1] - cuts[j]
        origin = along(-d * (step + (1 if received else 0)))
        block = held.at[origin, pl.ds(low, size)]
        return pltpu.make_async_remote_copy(
            src_ref=block, dst_ref=block,
            send_sem=ring_send.at[j, step], recv_sem=ring_recv.at[j, step],
            device_id={"freq": right if d == 1 else left}, device_id_type=MESH,
        )

    width = group * 2 * sites

    def sort_tiles(j):
        for chunk in range(cuts[j], cuts[j + 1]):
            low = chunk * width
            size = min(width, tiles.shape[0] - low)
            turned = lax.dot_general(
                tiles[low:low + size, :], sorter[:size, :], (((0,), (0,)), ((), ())),
                preferred_element_type=jnp.float32,
            )
            held[me_f, chunk] = jnp.where(slot_facts[1] > 0.5, turned, 0.0).astype(jnp.bfloat16)

    for at, j in enumerate(pieces):
        sort_tiles(j)
        if at == 0:
            pl.semaphore_wait(barrier, 2 + sens_size - 1)
        else:
            ring_copy(0, pieces[at - 1], False).start()

    lane = lax.broadcasted_iota(jnp.int32, (rows, LANES), 1)
    which = (lane % HALF) // sites
    sign = jnp.where(lane < HALF, -1.0, 1.0).astype(jnp.float32)
    spread[...] = jnp.zeros_like(spread)

    def transform(r):
        for c in range(2):
            value = lax.dot_general(
                forward[c], samples[r], (((1,), (1,)), ((), ())),
                preferred_element_type=jnp.float32,
            )
            for tile in range(lane_tiles):
                part = value[:, tile * LANES:min(slots, (tile + 1) * LANES)]
                if part.shape[1] < LANES:
                    part = jnp.concatenate(
                        [part, jnp.zeros((part.shape[0], LANES - part.shape[1]), part.dtype)], axis=1
                    )
                spectra[tile, pl.ds(c * rows + r, part.shape[0], stride=per_bin), :] = part

    def contract(step, j):
        origin = along(-sign_of[j] * step)
        for chunk in range(cuts[j], cuts[j + 1]):
            at = origin * chunks + chunk
            weights = held[origin, chunk]
            first = pl.multiple_of(at * (group * per_bin), group * per_bin)
            parts = [spectra[tile, pl.ds(first, group * per_bin), :] for tile in range(lane_tiles)]
            spec = jnp.concatenate(parts, axis=1)[:, :slots].astype(jnp.bfloat16)
            product = jnp.dot(spec, weights, preferred_element_type=jnp.float32)
            picked = [product[c * rows:(c + 1) * rows] for c in range(2)]
            for i in range(1, group):
                for c in range(2):
                    low = i * per_bin + c * rows
                    picked[c] = jnp.where(which == i, product[low:low + rows], picked[c])
            value = picked[0] + sign * pltpu.roll(picked[1], HALF, 1)
            z_own[pl.ds(pl.multiple_of(at * rows, rows), rows), :] = value
            z_send[at] = value.astype(jnp.bfloat16)
            wide = weights.astype(jnp.float32)
            power = wide * wide * slot_facts[0]
            total = power.reshape(slots // 8, 8, LANES).sum(axis=0)
            spread[...] += total * noise_weight[pl.ds(at, 1), :]

    def z_copies(step, j):
        origin = along(-sign_of[j] * step)
        part = pl.ds(origin * chunks + cuts[j], cuts[j + 1] - cuts[j])
        return [
            pltpu.make_async_remote_copy(
                src_ref=z_send.at[part], dst_ref=z_recv.at[d - 1, part],
                send_sem=z_send_sem.at[d - 1, step * count + j],
                recv_sem=z_recv_sem.at[d - 1, step * count + j],
                device_id={"sens": lax.rem(me_s + d, sens_size)}, device_id_type=MESH,
            )
            for d in range(1, sens_size)
        ]

    def receive(step, j, last):
        ring_copy(step, j, True).wait_recv()
        if not last:
            ring_copy(step + 1, j, False).start()

    def send_z(step, j):
        for copy in z_copies(step, j):
            copy.start()

    def transforms(low, high):
        lax.fori_loop(low, high, lambda r, carry: (transform(r), carry)[1], 0)

    ring_copy(0, pieces[-1], False).start()
    turns = 2 * len(pieces)
    done = 0
    for turn in range(turns):
        receive(turn // len(pieces), pieces[turn % len(pieces)], False)
        upto = rows * (turn + 1) // turns
        transforms(done, upto)
        done = upto

    def both(step, carry):
        for at, j in enumerate(pieces):
            receive(step, j, False)

            def one(arrival, inner):
                contract(arrival, j)
                return inner

            lax.fori_loop(2 * (step - 2), 2 * (step - 2) + 2, one, 0)
            for arrival in (2 * (step - 2), 2 * (step - 2) + 1):
                if at > 0:
                    send_z(arrival, pieces[at - 1])
                if at == len(pieces) - 1:
                    send_z(arrival, j)
        return carry

    lax.fori_loop(2, 5, both, 0)

    def single(step, carry):
        for at, j in enumerate(pieces):
            ring_copy(step, j, True).wait_recv()

            @pl.when(step < n - 2)
            def _():
                ring_copy(step + 1, j, False).start()

            contract(step + 1, j)
            if at > 0:
                send_z(step + 1, pieces[at - 1])
            if at == len(pieces) - 1:
                send_z(step + 1, j)
        return carry

    lax.fori_loop(5, n - 1, single, 0)
    spread_send[...] = spread[...]
    spread_copies = [
        pltpu.make_async_remote_copy(
            src_ref=spread_send, dst_ref=spread_recv.at[d - 1],
            send_sem=s_send_sem.at[d - 1], recv_sem=s_recv_sem.at[d - 1],
            device_id={"sens": lax.rem(me_s + d, sens_size)}, device_id_type=MESH,
        )
        for d in range(1, sens_size)
    ]
    for copy in spread_copies:
        copy.start()
    for step in range(n - 1):
        for j in pieces:
            ring_copy(step, j, False).wait_send()
    for step in range(n):
        for j in pieces:
            for copy in z_copies(step, j):
                copy.wait()
    for copy in spread_copies:
        copy.wait()
    total = spread[...]
    for d in range(1, sens_size):
        total += spread_recv[d - 1]
    total = jnp.broadcast_to(jnp.sum(total, axis=0, keepdims=True), total.shape)
    total = total + pltpu.roll(total, HALF, 1)
    folded = total
    for i in range(1, group):
        folded += pltpu.roll(total, LANES - i * sites, 1)
    spread[...] = folded

    def combine(at, carry):
        here = pl.ds(pl.multiple_of(at * rows, rows), rows)
        value = z_own[here, :]
        for d in range(1, sens_size):
            value += z_recv[d - 1, at].astype(jnp.float32)
        z_own[here, :] = value * cosine[pl.ds(at, 1), :] + pltpu.roll(value, HALF, 1) * sine[pl.ds(at, 1), :]
        return carry

    lax.fori_loop(0, all_chunks, combine, 0, unroll=4)

    seat = 32
    together = LANES // seat
    place = lax.broadcasted_iota(jnp.int32, (all_chunks, LANES), 1) // seat
    for base in range(0, rows, together):
        mine = [z_own[pl.ds(base + m, all_chunks, stride=rows), :] for m in range(together)]
        for c in range(2):
            for i in range(group):
                start = c * HALF + i * sites
                value = None
                for m in range(together):
                    moved = pltpu.roll(mine[m], (m * seat - start) % LANES, 1)
                    value = moved if value is None else jnp.where(place == m, moved, value)
                low = (c * group + i) * all_chunks
                gathered[low:low + all_chunks, base * seat:(base + together) * seat] = value.astype(jnp.bfloat16)
    result = lax.dot_general(
        gathered[...], inverse[...], (((0,), (0,)), ((), ())), preferred_element_type=jnp.float32
    )
    for r in range(rows):
        out[r] = result[r * seat:r * seat + sites].astype(jnp.bfloat16)


def on_device(freq_size, sens_size, samples, response_tiles, slot_sensor, sensor_noise, advance_offset):
    bins_dev, _, slots, sites = response_tiles.shape
    rows, _, step_count = samples.shape
    group = HALF // sites
    chunks = -(-bins_dev // group)
    all_chunks = freq_size * chunks
    period = 2 * freq_size * bins_dev
    bins, weight, forward, inverse = make_tables(freq_size, bins_dev, step_count, group, chunks)

    def per_lane(table):
        table = table.reshape(all_chunks, group * sites)
        table = jnp.pad(table, ((0, 0), (0, HALF - group * sites)))
        return jnp.concatenate([table, table], axis=1)

    live_slot = slot_sensor >= 0
    sensor_ids = lax.iota(jnp.int32, sensor_noise.shape[0])
    slot_noise = jnp.sum(
        jnp.where(slot_sensor[:, None] == sensor_ids[None, :], sensor_noise[None, :], jnp.float32(0.0)),
        axis=1,
    )
    slot_facts = jnp.stack([slot_noise, live_slot.astype(jnp.float32)])
    slot_facts = jnp.broadcast_to(slot_facts[:, :, None], (2, slots, LANES))
    tiles = response_tiles.transpose(0, 3, 1, 2).reshape(bins_dev * 2 * sites, slots)
    sorter = np.zeros((group, sites, 2, LANES), np.float32)
    for i, q, c in np.ndindex(group, sites, 2):
        sorter[i, q, c, c * HALF + i * sites + q] = 1.0
    sorter = jnp.asarray(sorter.reshape(group * sites * 2, LANES), jnp.bfloat16)

    turns = jnp.asarray(bins, jnp.int32)[:, None] * advance_offset[None, :] % period
    twiddle = turns.astype(jnp.float32) * (2.0 * math.pi / period)
    lane_sign = jnp.where(lax.iota(jnp.int32, LANES) < HALF, -1.0, 1.0).astype(jnp.float32)
    cosine = per_lane(jnp.cos(twiddle))
    sine = per_lane(jnp.sin(twiddle)) * lane_sign[None, :]
    noise_weight = per_lane(jnp.asarray(np.repeat(weight[:, None], sites, axis=1), jnp.float32))

    lane_tiles = -(-slots // LANES)
    peers = sens_size - 1
    count = 4 if peers * freq_size * 4 <= 1024 else 2
    vmem = pl.BlockSpec(memory_space=pltpu.VMEM)
    outlook, spread = pl.pallas_call(
        functools.partial(kernel, (freq_size, sens_size, chunks, group, sites, count)),
        out_shape=(
            jax.ShapeDtypeStruct((rows, sites, step_count), jnp.bfloat16),
            jax.ShapeDtypeStruct((8, LANES), jnp.float32),
        ),
        in_specs=[vmem] * 9,
        out_specs=(vmem, vmem),
        scratch_shapes=[
            pltpu.VMEM((freq_size, chunks, slots, LANES), jnp.bfloat16),
            pltpu.VMEM((lane_tiles, all_chunks * group * 2 * rows, LANES), jnp.float32),
            pltpu.VMEM((all_chunks * rows, LANES), jnp.float32),
            pltpu.VMEM((all_chunks, rows, LANES), jnp.bfloat16),
            pltpu.VMEM((peers, all_chunks, rows, LANES), jnp.bfloat16),
            pltpu.VMEM((2 * group * all_chunks, rows * 32), jnp.bfloat16),
            pltpu.VMEM((8, LANES), jnp.float32),
            pltpu.VMEM((peers, 8, LANES), jnp.float32),
            pltpu.SemaphoreType.DMA((count, freq_size - 1)),
            pltpu.SemaphoreType.DMA((count, freq_size - 1)),
            pltpu.SemaphoreType.DMA((peers, freq_size * count)),
            pltpu.SemaphoreType.DMA((peers, freq_size * count)),
            pltpu.SemaphoreType.DMA((peers,)),
            pltpu.SemaphoreType.DMA((peers,)),
        ],
        compiler_params=pltpu.CompilerParams(
            collective_id=0, has_side_effects=True, vmem_limit_bytes=60 * 1024 * 1024
        ),
    )(
        tiles, samples, jnp.asarray(forward, jnp.bfloat16), slot_facts, sorter, noise_weight,
        cosine, sine, jnp.asarray(inverse, jnp.bfloat16),
    )
    noise_spread = spread[0, :sites]
    return (outlook, noise_spread)


def solution(mesh):
    placed = (P("freq", "sens", None), P("freq", None, "sens", None), P("sens"), P(), P())
    return jax.shard_map(
        functools.partial(on_device, mesh.shape["freq"], mesh.shape["sens"]),
        mesh=mesh,
        in_specs=placed,
        out_specs=(P("freq", None, None), P()),
        check_vma=False,
    )
```

```python
import functools
import math

import jax
import jax.numpy as jnp
import numpy as np
from jax import lax
from jax.experimental import pallas as pl
from jax.experimental.pallas import tpu as pltpu
from jax.sharding import PartitionSpec as P

MESH = pl.DeviceIdType.MESH
HALF = 64
LANES = 128


def make_tables(freq_size, bins_dev, step_count, group, chunks):
    bin_count = freq_size * bins_dev
    period = 2 * bin_count
    slot = np.arange(freq_size * chunks * group)
    block, inside = slot // (chunks * group), slot % (chunks * group)
    live = (inside < bins_dev).astype(np.float64)
    bins = np.where(inside < bins_dev, block * bins_dev + inside, 0)
    turns = bins[:, None] * np.arange(step_count)[None, :] % period
    angle = turns * (2.0 * math.pi / period)
    forward = np.stack([np.cos(angle), -np.sin(angle)]) * live[None, :, None]
    weight = np.where(bins == 0, 1.0, 2.0) / period * live
    inverse = np.stack([np.cos(angle), -np.sin(angle)]) * weight[None, :, None]
    inverse = inverse.reshape(2, freq_size * chunks, group, step_count).transpose(0, 2, 1, 3)
    inverse = inverse.reshape(2 * group * freq_size * chunks, step_count)
    return bins, weight, forward, inverse


def kernel(
    dims,
    tiles, samples_in, forward_in, slot_ids, sensor_noise, sorter, noise_weight, bins, offsets, inverse_in,
    out, spread, samples, forward, inverse, slot_facts, cosine, sine, load_sem,
    held, spectra, z_own, z_send, z_recv, gathered, spread_send, spread_recv,
    ring_send, ring_recv, z_send_sem, z_recv_sem, s_send_sem, s_recv_sem,
):
    freq_size, sens_size, chunks, group, sites, count, period_of = dims
    rows, slots, step_count = samples_in.shape
    all_chunks = freq_size * chunks
    per_bin = 2 * rows
    lane_tiles = spectra.shape[0]
    me_f = lax.axis_index("freq")
    me_s = lax.axis_index("sens")
    n = freq_size

    def position_of(index):
        odd, pair = lax.rem(index, 2), index // 2
        return pair * (1 - odd) + (n - 1 - pair) * odd

    def index_of(position):
        high = position // (n // 2)
        return 2 * position * (1 - high) + (2 * (n - 1 - position) + 1) * high

    me_p = position_of(me_f)

    def along(step):
        return index_of(lax.rem(me_p + step + 2 * n, n))

    right, left = along(1), along(-1)
    barrier = pltpu.get_barrier_semaphore()
    for neighbour in (left, right):
        pl.semaphore_signal(barrier, inc=1, device_id={"freq": neighbour}, device_id_type=MESH)
    for d in range(1, sens_size):
        peer = lax.rem(me_s + d, sens_size)
        pl.semaphore_signal(barrier, inc=1, device_id={"sens": peer}, device_id_type=MESH)

    cuts = [chunks * i // count for i in range(count + 1)]
    cuts = [cut + cut % 2 for cut in cuts[:-1]] + [chunks]
    edges = [cut * slots for cut in cuts[:-1]] + [held.shape[1]]
    half = count // 2
    pieces = [j for i in range(half) for j in (i, half + i) if cuts[j + 1] > cuts[j]]
    sign_of = (1,) * half + (-1,) * half

    def ring_copy(step, j, received):
        d = sign_of[j]
        low, size = edges[j], edges[j + 1] - edges[j]
        origin = along(-d * (step + (1 if received else 0)))
        block = held.at[origin, pl.ds(low, size)]
        return pltpu.make_async_remote_copy(
            src_ref=block, dst_ref=block,
            send_sem=ring_send.at[j, step], recv_sem=ring_recv.at[j, step],
            device_id={"freq": right if d == 1 else left}, device_id_type=MESH,
        )

    loads = [
        pltpu.make_async_copy(source, target, load_sem.at[at])
        for at, (source, target) in enumerate(
            ((forward_in, forward), (samples_in, samples), (inverse_in, inverse))
        )
    ]
    for load in loads:
        load.start()
    ids = slot_ids[...]
    same = ids == lax.broadcasted_iota(jnp.int32, (slots, sensor_noise.shape[1]), 1)
    found = jnp.sum(jnp.where(same, sensor_noise[...], 0.0), axis=1, keepdims=True)
    slot_facts[0] = jnp.broadcast_to(found, (slots, LANES))
    slot_facts[1] = jnp.broadcast_to((ids >= 0).astype(jnp.float32), (slots, LANES))
    width = group * 2 * sites

    def sort_tiles(j):
        for chunk in range(cuts[j], cuts[j + 1]):
            low = chunk * width
            size = min(width, tiles.shape[0] - low)
            turned = lax.dot_general(
                tiles[low:low + size, :], sorter[:size, :], (((0,), (0,)), ((), ())),
                preferred_element_type=jnp.float32,
            )
            held[me_f, chunk * slots:(chunk + 1) * slots] = jnp.where(slot_facts[1] > 0.5, turned, 0.0).astype(jnp.bfloat16)

    for at, j in enumerate(pieces):
        sort_tiles(j)
        if at == 0:
            pl.semaphore_wait(barrier, 2 + sens_size - 1)
        else:
            ring_copy(0, pieces[at - 1], False).start()

    lane = lax.broadcasted_iota(jnp.int32, (rows, LANES), 1)
    which = (lane % HALF) // sites
    sign = jnp.where(lane < HALF, -1.0, 1.0).astype(jnp.float32)
    spread[...] = jnp.zeros_like(spread)

    def transform(r):
        for c in range(2):
            value = lax.dot_general(
                forward[c], samples[r], (((1,), (1,)), ((), ())),
                preferred_element_type=jnp.float32,
            )
            for tile in range(lane_tiles):
                part = value[:, tile * LANES:min(slots, (tile + 1) * LANES)]
                if part.shape[1] < LANES:
                    part = jnp.concatenate(
                        [part, jnp.zeros((part.shape[0], LANES - part.shape[1]), part.dtype)], axis=1
                    )
                spectra[tile, pl.ds(c * rows + r, part.shape[0], stride=per_bin), :] = part

    def contract(step, j):
        origin = along(-sign_of[j] * step)
        for chunk in range(cuts[j], cuts[j + 1]):
            at = origin * chunks + chunk
            weights = held[origin, chunk * slots:(chunk + 1) * slots]
            first = pl.multiple_of(at * (group * per_bin), group * per_bin)
            parts = [spectra[tile, pl.ds(first, group * per_bin), :] for tile in range(lane_tiles)]
            spec = jnp.concatenate(parts, axis=1)[:, :slots].astype(jnp.bfloat16)
            product = jnp.dot(spec, weights, preferred_element_type=jnp.float32)
            picked = [product[c * rows:(c + 1) * rows] for c in range(2)]
            for i in range(1, group):
                for c in range(2):
                    low = i * per_bin + c * rows
                    picked[c] = jnp.where(which == i, product[low:low + rows], picked[c])
            value = picked[0] + sign * pltpu.roll(picked[1], HALF, 1)
            z_own[pl.ds(pl.multiple_of(at * rows, rows), rows), :] = value
            z_send[at] = value.astype(jnp.bfloat16)
            wide = weights.astype(jnp.float32)
            power = wide * wide * slot_facts[0]
            total = power.reshape(slots // 8, 8, LANES).sum(axis=0)
            spread[...] += total * noise_weight[pl.ds(at, 1), :]

    def z_copies(step, j):
        origin = along(-sign_of[j] * step)
        part = pl.ds(origin * chunks + cuts[j], cuts[j + 1] - cuts[j])
        return [
            pltpu.make_async_remote_copy(
                src_ref=z_send.at[part], dst_ref=z_recv.at[d - 1, part],
                send_sem=z_send_sem.at[d - 1, step * count + j],
                recv_sem=z_recv_sem.at[d - 1, step * count + j],
                device_id={"sens": lax.rem(me_s + d, sens_size)}, device_id_type=MESH,
            )
            for d in range(1, sens_size)
        ]

    def receive(step, j, last):
        ring_copy(step, j, True).wait_recv()
        if not last:
            ring_copy(step + 1, j, False).start()

    def send_z(step, j):
        for copy in z_copies(step, j):
            copy.start()

    def transforms(low, high):
        lax.fori_loop(low, high, lambda r, carry: (transform(r), carry)[1], 0)

    ring_copy(0, pieces[-1], False).start()
    period = float(period_of)
    ahead = bins[...] * offsets[...]
    angle = (ahead - period * jnp.floor(ahead / period)) * (2.0 * math.pi / period)
    side = lax.broadcasted_iota(jnp.int32, angle.shape, 1)
    cosine[...] = jnp.cos(angle)
    sine[...] = jnp.sin(angle) * jnp.where(side < HALF, -1.0, 1.0)
    for load in loads:
        load.wait()
    turns = 2 * len(pieces)
    done = 0
    for turn in range(turns):
        receive(turn // len(pieces), pieces[turn % len(pieces)], False)
        upto = rows * (turn + 1) // turns
        transforms(done, upto)
        done = upto

    def both(step, carry):
        for at, j in enumerate(pieces):
            receive(step, j, False)

            def one(arrival, inner):
                contract(arrival, j)
                return inner

            lax.fori_loop(2 * (step - 2), 2 * (step - 2) + 2, one, 0)
            for arrival in (2 * (step - 2), 2 * (step - 2) + 1):
                if at > 0:
                    send_z(arrival, pieces[at - 1])
                if at == len(pieces) - 1:
                    send_z(arrival, j)
        return carry

    lax.fori_loop(2, 5, both, 0)

    def single(step, carry):
        for at, j in enumerate(pieces):
            ring_copy(step, j, True).wait_recv()

            @pl.when(step < n - 2)
            def _():
                ring_copy(step + 1, j, False).start()

            contract(step + 1, j)
            if at > 0:
                send_z(step + 1, pieces[at - 1])
            if at == len(pieces) - 1:
                send_z(step + 1, j)
        return carry

    lax.fori_loop(5, n - 1, single, 0)
    spread_send[...] = spread[...]
    spread_copies = [
        pltpu.make_async_remote_copy(
            src_ref=spread_send, dst_ref=spread_recv.at[d - 1],
            send_sem=s_send_sem.at[d - 1], recv_sem=s_recv_sem.at[d - 1],
            device_id={"sens": lax.rem(me_s + d, sens_size)}, device_id_type=MESH,
        )
        for d in range(1, sens_size)
    ]
    for copy in spread_copies:
        copy.start()
    for step in range(n - 1):
        for j in pieces:
            ring_copy(step, j, False).wait_send()
    for step in range(n):
        for j in pieces:
            for copy in z_copies(step, j):
                copy.wait()
    for copy in spread_copies:
        copy.wait()
    total = spread[...]
    for d in range(1, sens_size):
        total += spread_recv[d - 1]
    total = jnp.broadcast_to(jnp.sum(total, axis=0, keepdims=True), total.shape)
    total = total + pltpu.roll(total, HALF, 1)
    folded = total
    for i in range(1, group):
        folded += pltpu.roll(total, LANES - i * sites, 1)
    spread[...] = folded

    def combine(at, carry):
        here = pl.ds(pl.multiple_of(at * rows, rows), rows)
        value = z_own[here, :]
        for d in range(1, sens_size):
            value += z_recv[d - 1, at].astype(jnp.float32)
        z_own[here, :] = value * cosine[pl.ds(at, 1), :] + pltpu.roll(value, HALF, 1) * sine[pl.ds(at, 1), :]
        return carry

    lax.fori_loop(0, all_chunks, combine, 0, unroll=4)

    seat = 32
    together = LANES // seat
    place = lax.broadcasted_iota(jnp.int32, (all_chunks, LANES), 1) // seat
    for base in range(0, rows, together):
        mine = [z_own[pl.ds(base + m, all_chunks, stride=rows), :] for m in range(together)]
        for c in range(2):
            for i in range(group):
                start = c * HALF + i * sites
                value = None
                for m in range(together):
                    moved = pltpu.roll(mine[m], (m * seat - start) % LANES, 1)
                    value = moved if value is None else jnp.where(place == m, moved, value)
                low = (c * group + i) * all_chunks
                gathered[low:low + all_chunks, base * seat:(base + together) * seat] = value.astype(jnp.bfloat16)
    result = lax.dot_general(
        gathered[...], inverse[...], (((0,), (0,)), ((), ())), preferred_element_type=jnp.float32
    )
    for r in range(rows):
        out[r] = result[r * seat:r * seat + sites].astype(jnp.bfloat16)


def on_device(freq_size, sens_size, samples, response_tiles, slot_sensor, sensor_noise, advance_offset):
    bins_dev, _, slots, sites = response_tiles.shape
    rows, _, step_count = samples.shape
    group = HALF // sites
    chunks = -(-bins_dev // group)
    all_chunks = freq_size * chunks
    period = 2 * freq_size * bins_dev
    bins, weight, forward, inverse = make_tables(freq_size, bins_dev, step_count, group, chunks)

    def per_lane(table):
        table = table.reshape(all_chunks, group * sites)
        table = np.pad(table, ((0, 0), (0, HALF - group * sites)))
        return jnp.asarray(np.concatenate([table, table], axis=1))

    tiles = response_tiles.transpose(0, 3, 1, 2).reshape(bins_dev * 2 * sites, slots)
    sorter = np.zeros((group, sites, 2, LANES), np.float32)
    for i, q, c in np.ndindex(group, sites, 2):
        sorter[i, q, c, c * HALF + i * sites + q] = 1.0
    sorter = jnp.asarray(sorter.reshape(group * sites * 2, LANES), jnp.bfloat16)

    offsets = jnp.tile(advance_offset.astype(jnp.float32), group)
    offsets = jnp.tile(jnp.pad(offsets, (0, HALF - group * sites)), 2)[None, :]
    lane_bins = per_lane(np.repeat(bins[:, None], sites, axis=1).astype(np.float32))
    noise_weight = per_lane(np.repeat(weight[:, None], sites, axis=1).astype(np.float32))

    lane_tiles = -(-slots // LANES)
    peers = sens_size - 1
    count = 4 if peers * freq_size * 4 <= 1024 else 2
    vmem = pl.BlockSpec(memory_space=pltpu.VMEM)
    anywhere = pl.BlockSpec(memory_space=pl.ANY)
    outlook, spread = pl.pallas_call(
        functools.partial(kernel, (freq_size, sens_size, chunks, group, sites, count, period)),
        out_shape=(
            jax.ShapeDtypeStruct((rows, sites, step_count), jnp.bfloat16),
            jax.ShapeDtypeStruct((8, LANES), jnp.float32),
        ),
        in_specs=[vmem, anywhere, anywhere] + [vmem] * 6 + [anywhere],
        out_specs=(vmem, vmem),
        scratch_shapes=[
            pltpu.VMEM(samples.shape, jnp.bfloat16),
            pltpu.VMEM(forward.shape, jnp.bfloat16),
            pltpu.VMEM(inverse.shape, jnp.bfloat16),
            pltpu.VMEM((2, slots, LANES), jnp.float32),
            pltpu.VMEM((all_chunks, LANES), jnp.float32),
            pltpu.VMEM((all_chunks, LANES), jnp.float32),
            pltpu.SemaphoreType.DMA((3,)),
            pltpu.VMEM((freq_size, -(-chunks * slots // 16) * 16, LANES), jnp.bfloat16),
            pltpu.VMEM((lane_tiles, all_chunks * group * 2 * rows, LANES), jnp.float32),
            pltpu.VMEM((all_chunks * rows, LANES), jnp.float32),
            pltpu.VMEM((all_chunks, rows, LANES), jnp.bfloat16),
            pltpu.VMEM((peers, all_chunks, rows, LANES), jnp.bfloat16),
            pltpu.VMEM((2 * group * all_chunks, rows * 32), jnp.bfloat16),
            pltpu.VMEM((8, LANES), jnp.float32),
            pltpu.VMEM((peers, 8, LANES), jnp.float32),
            pltpu.SemaphoreType.DMA((count, freq_size - 1)),
            pltpu.SemaphoreType.DMA((count, freq_size - 1)),
            pltpu.SemaphoreType.DMA((peers, freq_size * count)),
            pltpu.SemaphoreType.DMA((peers, freq_size * count)),
            pltpu.SemaphoreType.DMA((peers,)),
            pltpu.SemaphoreType.DMA((peers,)),
        ],
        compiler_params=pltpu.CompilerParams(
            collective_id=0, has_side_effects=True, vmem_limit_bytes=60 * 1024 * 1024
        ),
    )(
        tiles, samples, jnp.asarray(forward, jnp.bfloat16), slot_sensor[:, None], sensor_noise[None, :],
        sorter, noise_weight, lane_bins, offsets, jnp.asarray(inverse, jnp.bfloat16),
    )
    noise_spread = spread[0, :sites]
    return (outlook, noise_spread)


def solution(mesh):
    placed = (P("freq", "sens", None), P("freq", None, "sens", None), P("sens"), P(), P())
    return jax.shard_map(
        functools.partial(on_device, mesh.shape["freq"], mesh.shape["sens"]),
        mesh=mesh,
        in_specs=placed,
        out_specs=(P("freq", None, None), P()),
        check_vma=False,
    )
```
